32 devices in a mesh: energy: 16 (over z, x, core), space: 2 (over y).
Axes of the slice: x: 2, y: 2, z: 4, core: 2. Of those that a mesh axis runs over, the one named last changes fastest.
Arguments:
- g_lesser: float32 [2, 256, 2, 256, 256], P(None, 'energy', 'space'), may hold values from -6 to 6
- g_greater: float32 [2, 256, 2, 256, 256], P(None, 'energy', 'space'), may hold values from -6 to 6
- v_diag: float32 [2, 256, 256], P('space'), may hold values from -0.375 to 0.375
- v_upper: float32 [2, 256, 256], P('space'), may hold values from -0.375 to 0.375
Outputs:
- screened: float32 [2, 64, 2, 256, 256], P(None, 'energy', 'space')
The draws below stay inside these ranges and needn't reach their ends.
All inputs are finite; a program needn't handle non-finite values.
Results may differ from the reference program's by a relative error of at most 0.000098.
Values sent between devices are 32-bit elements; how exact they have to be, the bound alone decides.
A program may use at most 128 MiB of HBM per device.

```python
import math
import jax
import jax.numpy as jnp
from jax import lax

NE = 256
NW = 64
B = 256
NB = 2


def steps_of(rng, shape, shards, smallest, top_value):
    level, own = 1.0, jax.random.fold_in(rng, 6)
    for dim, parts in shards:
        heights = jnp.exp(jax.random.uniform(jax.random.fold_in(own, dim), (parts,), jnp.float32, smallest / len(shards), top_value / len(shards)))
        level = level * jnp.repeat(heights, shape[dim] // parts).reshape([-1 if axis == dim else 1 for axis in range(len(shape))])
    return level


def scatter_about(rng, extent, width, limit, shards=(), kind=jnp.bfloat16):
    drawn = width * jax.random.normal(rng, extent, jnp.float32)
    if shards:
        drawn = drawn * steps_of(rng, extent, shards, -0.22, 0.18)
    return jnp.clip(drawn, -limit, limit).astype(kind)


def setup_inputs(seed: int = 0) -> dict:
    key_of = jax.random.split(jax.random.key(seed), 5)
    return {
        "g_lesser": scatter_about(key_of[0], (2, NE, NB, B, B), 1.0, 6.0, ((1, 16), (2, 2)), jnp.float32),
        "g_greater": scatter_about(key_of[1], (2, NE, NB, B, B), 1.0, 6.0, ((1, 16), (2, 2)), jnp.float32),
        "v_diag": scatter_about(key_of[2], (NB, B, B), B ** -0.5, 0.375, ((0, 2),), jnp.float32),
        "v_upper": scatter_about(key_of[3], (NB, B, B), B ** -0.5, 0.375, ((0, 2),), jnp.float32),
    }


prefactor = 0.0625


def tables(count):
    length = 2 * count
    freqs = jnp.arange(length, dtype=jnp.int32)[:, None]
    points = jnp.arange(count, dtype=jnp.int32)[None, :]
    phase = (2.0 * math.pi / length) * ((freqs * points) % length).astype(jnp.float32)
    return jnp.cos(phase), jnp.sin(phase)


def product(left, right):
    return jnp.dot(left, right, precision=lax.Precision.HIGHEST, preferred_element_type=jnp.float32)


def correlate(lesser, greater, keep):
    count = lesser.shape[1]
    rest = tuple(lesser.shape[2:])
    lesser = lesser.reshape(2, count, -1)
    greater = greater.reshape(2, count, -1)
    cosine, sine = tables(count)
    less_re = product(cosine, lesser[0]) + product(sine, lesser[1])
    less_im = product(cosine, lesser[1]) - product(sine, lesser[0])
    great_re = product(cosine, greater[0]) - product(sine, greater[1])
    great_im = product(cosine, greater[1]) + product(sine, greater[0])
    spec_re = less_re * great_re - less_im * great_im
    spec_im = less_re * great_im + less_im * great_re
    factor = prefactor / (2 * count)
    back_cos = cosine.T[:keep]
    back_sin = sine.T[:keep]
    out_re = (product(back_cos, spec_re) - product(back_sin, spec_im)) * factor
    out_im = (product(back_cos, spec_im) + product(back_sin, spec_re)) * factor
    return jnp.stack([out_re, out_im]).reshape((2, keep) + rest)


def sandwich(left, middle, right):
    halfway = jnp.einsum('rab,...rbd->...rad', left, middle, precision=lax.Precision.HIGHEST)
    return jnp.einsum('...rad,rdf->...raf', halfway, right, precision=lax.Precision.HIGHEST)


def reference(g_lesser, g_greater, v_diag, v_upper):
    flipped = jnp.swapaxes(g_greater, 3, 4)

    def one_row(pair):
        return correlate(pair[0], pair[1], NW)

    rows = lax.map(one_row, (jnp.moveaxis(g_lesser, 2, 0), jnp.moveaxis(flipped, 2, 0)))
    polar = jnp.moveaxis(rows, 0, 2)
    uppers_before = jnp.concatenate([jnp.zeros((1,) + tuple(v_upper.shape[1:]), jnp.float32), v_upper[:-1]], axis=0)
    upper_swapped = jnp.swapaxes(v_upper, 1, 2)
    before_swapped = jnp.swapaxes(uppers_before, 1, 2)

    def one_energy(block):
        padded = jnp.pad(block, ((0, 0), (1, 1), (0, 0), (0, 0)))
        own_term = sandwich(v_diag, block, v_diag)
        above_term = sandwich(before_swapped, padded[:, :-2], uppers_before)
        below_term = sandwich(v_upper, padded[:, 2:], upper_swapped)
        return own_term + above_term + below_term

    result = lax.map(one_energy, jnp.moveaxis(polar, 1, 0))
    return jnp.moveaxis(result, 0, 1)
```

```python
import functools
import math

import jax
import jax.numpy as jnp
import numpy as np
from jax import lax
from jax.experimental import pallas as pl
from jax.experimental.pallas import tpu as pltpu
from jax.sharding import PartitionSpec as P

NW = 64
PREFACTOR = 0.0625
ROWS = 8
LANES = 128
AHEAD = 3
HIGH = lax.Precision.HIGH


def split_np(table):
    table = np.asarray(table, np.float64)
    high = table.astype(jnp.bfloat16)
    low = (table - high.astype(np.float64)).astype(jnp.bfloat16)
    return np.concatenate([high, low, high], axis=1)


def tables(keep):
    length = 2 * keep

    def forward(start, sign):
        phase = 2.0 * math.pi / length * (np.outer(np.arange(length), np.arange(start, start + keep)) % length)
        cos, sin = np.cos(phase), sign * np.sin(phase)
        return np.block([[cos, sin], [-sin, cos]])

    phase = 2.0 * math.pi / length * (np.outer(np.arange(keep), np.arange(length)) % length)
    cos, sin = np.cos(phase) * (PREFACTOR / length), np.sin(phase) * (PREFACTOR / length)
    back = np.block([[cos, -sin], [sin, cos]])
    wide = [np.concatenate([forward(0, sign), forward(keep, sign)], axis=1) for sign in (1, -1)]
    narrow = [forward(0, sign) for sign in (1, -1)]
    return [jnp.asarray(t) for t in (
        np.stack([split_np(t) for t in wide]), np.stack([split_np(t) for t in narrow]), split_np(back))]


def stacked(value):
    high = value.astype(jnp.bfloat16)
    low = (value - high.astype(jnp.float32)).astype(jnp.bfloat16)
    return jnp.concatenate([high, high, low], axis=0)


def dot(table, value):
    return jnp.dot(table, stacked(value), preferred_element_type=jnp.float32)


def correlate_kernel(
    n, group, rows, wide_tab, narrow_tab, back_tab, less, great, out, near,
    in_buf, halo_buf, polar_buf, chain_buf, final_buf,
    in_send, in_recv, own_sem, halo_send, halo_recv, chain_send, chain_recv,
    out_send, out_recv, out_own, near_send, near_recv,
):
    me = lax.axis_index("energy")
    mine, share = me // group, lax.rem(me, group)
    groups = n // group
    last = groups - 1
    sources = (less, great)
    held = less.shape[1]
    tiles = less.shape[3]
    row = lax.axis_index("space")
    sides = near.shape[0]
    stages = in_buf.shape[1]
    keep = in_buf.shape[3]
    kept = out.shape[1]
    block = group * kept
    mesh_id = pl.DeviceIdType.MESH

    def lanes_of(q):
        return pl.ds(pl.multiple_of(q // tiles * LANES, LANES), LANES)

    def in_copy(k, q, d):
        other = lax.rem(share + d, group)
        return pltpu.make_async_remote_copy(
            src_ref=sources[k].at[:, :, other, lax.rem(q, tiles), :, lanes_of(q)],
            dst_ref=in_buf.at[k, q, :, pl.ds(share * held, held)],
            send_sem=in_send.at[k, q, d],
            recv_sem=in_recv.at[k, q, d],
            device_id={"energy": mine * group + other},
            device_id_type=mesh_id,
        )

    def in_own(k, q):
        return pltpu.make_async_copy(
            sources[k].at[:, :, share, lax.rem(q, tiles), :, lanes_of(q)],
            in_buf.at[k, q, :, pl.ds(share * held, held)],
            own_sem.at[k, q],
        )

    def pivot(q):
        return lax.rem(q, groups)

    def halo_copy(k, q):
        peer = lax.rem(me + (group if k else n - group), n)
        return pltpu.make_async_remote_copy(
            src_ref=in_buf.at[k, q],
            dst_ref=halo_buf.at[q],
            send_sem=halo_send.at[k, q],
            recv_sem=halo_recv.at[q],
            device_id={"energy": peer},
            device_id_type=mesh_id,
        )

    def halo_sends(k, q):
        if k:
            return jnp.logical_and(mine >= pivot(q), mine < last)
        return jnp.logical_and(mine <= pivot(q), mine > 0)

    def chain_copy(up, q, j):
        peer = lax.rem(me + (group if up else n - group), n)
        return pltpu.make_async_remote_copy(
            src_ref=polar_buf.at[q, :, pl.ds(j * block, block)],
            dst_ref=chain_buf.at[q, j + up],
            send_sem=chain_send.at[up, q, j],
            recv_sem=chain_recv.at[up, q, j],
            device_id={"energy": peer},
            device_id_type=mesh_id,
        )

    def out_copy(q, d):
        other = lax.rem(share + d, group)
        return pltpu.make_async_remote_copy(
            src_ref=polar_buf.at[q, :, pl.ds((mine * group + other) * kept, kept)],
            dst_ref=final_buf.at[q, :, :, share],
            send_sem=out_send.at[q, d],
            recv_sem=out_recv.at[q, d],
            device_id={"energy": mine * group + other},
            device_id_type=mesh_id,
        )

    def out_mine(q):
        return pltpu.make_async_copy(
            final_buf.at[q], out.at[:, :, :, lax.rem(q, tiles), :, lanes_of(q)], out_own.at[q])

    def near_copy(side, q):
        return pltpu.make_async_remote_copy(
            src_ref=final_buf.at[q],
            dst_ref=near.at[side, :, :, :, lax.rem(q, tiles), :, lanes_of(q)],
            send_sem=near_send.at[side, q],
            recv_sem=near_recv.at[side, q],
            device_id={"space": lax.rem(row + (rows - 1 if side else 1), rows)},
            device_id_type=mesh_id,
        )

    def near_if(side, receiving, body):
        if rows == 2:
            body()
        else:
            pl.when(row > 0 if side != receiving else row < rows - 1)(body)

    def each(first, last, body):
        def step(d, carry):
            body(d)
            return carry
        lax.fori_loop(first, last, step, 0)

    barrier = pltpu.get_barrier_semaphore()
    each(1, n, lambda d: pl.semaphore_signal(
        barrier, inc=1, device_id={"energy": lax.rem(me + d, n)}, device_id_type=mesh_id))
    for side in range(sides):
        pl.semaphore_signal(
            barrier, inc=1, device_id={"space": lax.rem(row + (rows - 1 if side else 1), rows)}, device_id_type=mesh_id)
    pl.semaphore_wait(barrier, n - 1 + sides)

    def send_stage(q):
        for k in range(2):
            in_own(k, q).start()
            each(1, group, lambda d: in_copy(k, q, d).start())

    def forward_stage(q):
        for k in range(2):
            in_own(k, q).wait()
            each(1, group, lambda d: in_copy(k, q, d).wait_recv())

            @pl.when(halo_sends(k, q))
            def _():
                halo_copy(k, q).start()

    def pair(tile, i):
        return jnp.concatenate([tile[:, :, i + s].reshape(2 * keep, LANES) for s in range(2)], axis=1)

    def compute_stage(q):
        alone = mine == pivot(q)

        @pl.when(jnp.logical_not(alone))
        def _():
            halo_copy(0, q).wait_recv()

        @pl.when(alone)
        def _():
            halo_buf[q] = jnp.zeros(halo_buf.shape[1:], jnp.float32)

        wide = jnp.where(mine > pivot(q), 1, 0)
        for i in range(0, ROWS, 2):
            own = pair(in_buf.at[wide, q], i)
            other = pair(in_buf.at[1 - wide, q], i)
            halo = pair(halo_buf.at[q], i)
            spec_a = dot(wide_tab[wide], jnp.concatenate([own, halo], axis=0))
            spec_b = dot(narrow_tab[1 - wide], other)
            mid = spec_a.shape[0] // 2
            ar, ai, br, bi = spec_a[:mid], spec_a[mid:], spec_b[:mid], spec_b[mid:]
            spec = jnp.concatenate([ar * br - ai * bi, ar * bi + ai * br], axis=0)
            polar = dot(back_tab[...], spec)
            for s in range(2):
                polar_buf[q, :, :, i + s] = polar[:, s * LANES:(s + 1) * LANES].reshape(2, keep, LANES)

    def add_block(up, q, j):
        here = pl.ds(j * block, block)
        polar_buf[q, :, here] = polar_buf[q, :, here] + chain_buf[q, j + up]

    def chain_stage(up, q):
        far = 0 if up else last

        def hop(j):
            @pl.when(mine != far)
            def _():
                chain_copy(up, q, j).wait_recv()
                add_block(up, q, j)

            @pl.when(mine != j)
            def _():
                chain_copy(up, q, j).start()

        if up:
            each(0, last - mine + 1, lambda t: hop(last - t))
        else:
            each(0, mine + 1, hop)

    def final_stage(q):
        final_buf[q, :, :, share] = polar_buf[q, :, pl.ds(me * kept, kept)]
        each(1, group, lambda d: out_copy(q, d).start())

    def near_stage(q):
        each(1, group, lambda d: out_copy(q, d).wait_recv())
        for side in range(sides):
            near_if(side, False, lambda: near_copy(side, q).start())
        out_mine(q).start()

    def at(q, body):
        pl.when(jnp.logical_and(q >= 0, q < stages))(lambda: body(q))

    each(0, min(AHEAD, stages), send_stage)
    below = last - mine
    late = jnp.maximum(mine, below)

    def step(i):
        at(i + AHEAD, send_stage)
        at(i, forward_stage)
        at(i - 1, compute_stage)
        at(i - 1 - mine, lambda q: chain_stage(1, q))
        at(i - 1 - below, lambda q: chain_stage(0, q))
        at(i - 1 - late, final_stage)
        at(i - 2 - late - AHEAD, near_stage)

    each(0, stages + 2 + last + AHEAD, step)

    def finish(q):
        out_mine(q).wait()
        for side in range(sides):
            near_if(side, False, lambda: near_copy(side, q).wait_send())
            near_if(side, True, lambda: near_copy(side, q).wait_recv())
        for k in range(2):
            each(1, group, lambda d: in_copy(k, q, d).wait_send())

            @pl.when(halo_sends(k, q))
            def _():
                halo_copy(k, q).wait_send()
        each(mine + 1, groups, lambda j: chain_copy(1, q, j).wait_send())
        each(0, mine, lambda j: chain_copy(0, q, j).wait_send())
        each(1, group, lambda d: out_copy(q, d).wait_send())

    each(0, stages, finish)


def polarization(g_lesser, g_flipped, keep):
    n, rows = lax.axis_size("energy"), lax.axis_size("space")
    sides = 1 if rows == 2 else 2
    _, held, _, size, width = g_lesser.shape
    group = keep // held
    groups = n // group
    tiles = size // group // ROWS
    stages = tiles * (width // LANES)
    less = g_lesser.reshape(2, held, group, tiles, ROWS, width)
    great = g_flipped.reshape(2, held, group, tiles, ROWS, width)
    tabs = tables(keep)
    any_spec = pl.BlockSpec(memory_space=pl.ANY)
    dma = pltpu.SemaphoreType.DMA
    tile = (ROWS, LANES)
    kept = keep // n
    shape = (2, kept, group, tiles, ROWS, width)

    def vmem(*dims):
        return pltpu.VMEM(dims + tile, jnp.float32)

    out, near = pl.pallas_call(
        functools.partial(correlate_kernel, n, group, rows),
        out_shape=[jax.ShapeDtypeStruct(s, jnp.float32) for s in (shape, (sides,) + shape)],
        in_specs=[pl.BlockSpec(memory_space=pltpu.VMEM)] * len(tabs) + [any_spec] * 2,
        out_specs=[any_spec] * 2,
        scratch_shapes=[
            vmem(2, stages, 2, keep), vmem(stages, 2, keep), vmem(stages, 2, keep),
            vmem(stages, groups + 1, 2, group * kept), vmem(stages, 2, kept, group),
            dma((2, stages, group)), dma((2, stages, group)), dma((2, stages)),
            dma((2, stages)), dma((stages,)),
            dma((2, stages, groups)), dma((2, stages, groups)),
            dma((stages, group)), dma((stages, group)), dma((stages,)),
            dma((sides, stages)), dma((sides, stages)),
        ],
        compiler_params=pltpu.CompilerParams(
            collective_id=0, has_side_effects=True, vmem_limit_bytes=60 * 2**20),
    )(*tabs, less, great)
    return out.reshape(2, kept, size, width), near.reshape(sides, 2, kept, size, width)


def shifted(block, axis, distance):
    devices = range(lax.axis_size(axis))
    return lax.ppermute(block, axis, [(i - distance, i) for i in devices if i - distance in devices])


def sandwich(left, middle, right):
    halfway = jnp.einsum("ab,cwbd->cwad", left, middle, precision=HIGH)
    return jnp.einsum("cwad,df->cwaf", halfway, right, precision=HIGH)


def local(g_lesser, g_greater, v_diag, v_upper):
    polar, near = polarization(g_lesser, jnp.swapaxes(g_greater, 3, 4), NW)
    rows = lax.axis_size("space")
    before = shifted(v_upper, "space", 1)[0]
    diag, upper = v_diag[0], v_upper[0]
    if rows == 2:
        coupling = jnp.where(lax.axis_index("space") == 0, upper, before.T)
        total = sandwich(diag, polar, diag) + sandwich(coupling, near[0], coupling.T)
    else:
        row = lax.axis_index("space")
        above = jnp.where(row > 0, near[0], 0.0)
        below = jnp.where(row < rows - 1, near[1], 0.0)
        total = sandwich(diag, polar, diag)
        total = total + sandwich(before.T, above, before) + sandwich(upper, below, upper.T)
    return total[:, :, None]


def solution(mesh):
    in_specs = (
        P(None, "energy", "space", None, None),
        P(None, "energy", "space", None, None),
        P("space", None, None),
        P("space", None, None),
    )
    out_specs = P(None, "energy", "space", None, None)
    return jax.shard_map(local, mesh=mesh, in_specs=in_specs, out_specs=out_specs, check_vma=False)
```

```python
import functools
import math

import jax
import jax.numpy as jnp
import numpy as np
from jax import lax
from jax.experimental import pallas as pl
from jax.experimental.pallas import tpu as pltpu
from jax.sharding import PartitionSpec as P

NW = 64
PREFACTOR = 0.0625
ROWS = 8
LANES = 128
AHEAD = 2
PART = 64
SLOTS = 4


def split_np(table):
    table = np.asarray(table, np.float64)
    high = table.astype(jnp.bfloat16)
    low = (table - high.astype(np.float64)).astype(jnp.bfloat16)
    return np.concatenate([high, low, high], axis=1)


def tables(keep):
    length = 2 * keep

    def forward(start, sign):
        phase = 2.0 * math.pi / length * (np.outer(np.arange(length), np.arange(start, start + keep)) % length)
        cos, sin = np.cos(phase), sign * np.sin(phase)
        return np.block([[cos, sin], [-sin, cos]])

    phase = 2.0 * math.pi / length * (np.outer(np.arange(keep), np.arange(length)) % length)
    cos, sin = np.cos(phase) * (PREFACTOR / length), np.sin(phase) * (PREFACTOR / length)
    back = np.block([[cos, -sin], [sin, cos]])
    wide = [np.concatenate([forward(0, sign), forward(keep, sign)], axis=1) for sign in (1, -1)]
    narrow = [forward(0, sign) for sign in (1, -1)]
    return [jnp.asarray(t) for t in (
        np.stack([split_np(t) for t in wide]), np.stack([split_np(t) for t in narrow]), split_np(back))]


def split(value):
    high = value.astype(jnp.bfloat16)
    return high, (value - high.astype(jnp.float32)).astype(jnp.bfloat16)


def stacked(value):
    high, low = split(value)
    return jnp.concatenate([high, high, low], axis=0)


def spread(value):
    high, low = split(value)
    return jnp.concatenate([high, low, high], axis=1)


def product(left, right):
    return jnp.dot(left, right, preferred_element_type=jnp.float32)


def dot(table, value):
    return product(table, stacked(value))


def screening_kernel(
    n, group, rows, wide_tab, narrow_tab, back_tab, diag, upper, less, great, out,
    raw_buf, flip_buf, in_buf, halo_buf, chain_buf, final_buf, near_buf, half_buf, total_buf,
    before_buf, right_tab, left_tab,
    raw_sem, in_send, in_recv, own_sem, halo_send, halo_recv, chain_send, chain_recv,
    out_send, out_recv, near_send, near_recv, edge_sem, result_sem,
):
    me = lax.axis_index("energy")
    mine, share = me // group, lax.rem(me, group)
    groups = n // group
    last = groups - 1
    row = lax.axis_index("space")
    held, size, width = great.shape[1:]
    tiles = less.shape[2]
    sides = near_buf.shape[0]
    stages = in_buf.shape[1]
    keep = in_buf.shape[3]
    count = out.shape[0]
    kept = count // 2
    block = group * kept
    parts = left_tab.shape[0]
    per_part = tiles // parts
    mesh_id = pl.DeviceIdType.MESH

    def each(first, last, body):
        def step(d, carry):
            body(d)
            return carry
        lax.fori_loop(first, last, step, 0)

    def raw_copy(u):
        half, rest = u // (2 * held), lax.rem(u, 2 * held)
        slot = lax.rem(u, SLOTS)
        return pltpu.make_async_copy(
            great.at[rest // held, lax.rem(rest, held), pl.ds(pl.multiple_of(half * LANES, LANES), LANES)],
            raw_buf.at[slot], raw_sem.at[slot])

    def flip_half(half):
        first = half * 2 * held

        def flip(r):
            u = first + r
            raw_copy(u).wait()
            flip_buf[half, r // held, lax.rem(r, held)] = raw_buf[lax.rem(u, SLOTS)].T.reshape(
                tiles, group, ROWS, LANES)

            @pl.when(u + SLOTS < 2 * held * (width // LANES))
            def _():
                raw_copy(u + SLOTS).start()

        each(0, 2 * held, flip)

    def source(k, q, other):
        half, tile = q // tiles, lax.rem(q, tiles)
        if k:
            return flip_buf.at[half, :, :, tile, other]
        return less.at[:, :, tile, other, :, pl.ds(pl.multiple_of(half * LANES, LANES), LANES)]

    def in_copy(k, q, d):
        other = lax.rem(share + d, group)
        return pltpu.make_async_remote_copy(
            src_ref=source(k, q, other),
            dst_ref=in_buf.at[k, q, :, pl.ds(share * held, held)],
            send_sem=in_send.at[k, q, d],
            recv_sem=in_recv.at[k, q, d],
            device_id={"energy": mine * group + other},
            device_id_type=mesh_id,
        )

    def in_own(k, q):
        return pltpu.make_async_copy(
            source(k, q, share), in_buf.at[k, q, :, pl.ds(share * held, held)], own_sem.at[k, q])

    def pivot(q):
        return lax.rem(q, groups)

    def halo_copy(k, q):
        peer = lax.rem(me + (group if k else n - group), n)
        return pltpu.make_async_remote_copy(
            src_ref=in_buf.at[k, q],
            dst_ref=halo_buf.at[q],
            send_sem=halo_send.at[k, q],
            recv_sem=halo_recv.at[q],
            device_id={"energy": peer},
            device_id_type=mesh_id,
        )

    def halo_sends(k, q):
        if k:
            return jnp.logical_and(mine >= pivot(q), mine < last)
        return jnp.logical_and(mine <= pivot(q), mine > 0)

    def polar_slot(q):
        return jnp.where(jnp.logical_or(mine < pivot(q), mine == last), 1, 0)

    def slot_sent(q):
        return jnp.logical_and(mine == pivot(q), jnp.logical_and(mine > 0, mine < last))

    def chain_copy(up, q, j):
        peer = lax.rem(me + (group if up else n - group), n)
        return pltpu.make_async_remote_copy(
            src_ref=in_buf.at[polar_slot(q), q, :, pl.ds(j * block, block)],
            dst_ref=chain_buf.at[q, j + up],
            send_sem=chain_send.at[up, q, j],
            recv_sem=chain_recv.at[up, q, j],
            device_id={"energy": peer},
            device_id_type=mesh_id,
        )

    def out_copy(q, d):
        other = lax.rem(share + d, group)
        return pltpu.make_async_remote_copy(
            src_ref=in_buf.at[polar_slot(q), q, :, pl.ds((mine * group + other) * kept, kept)],
            dst_ref=final_buf.at[q, :, :, share],
            send_sem=out_send.at[q, d],
            recv_sem=out_recv.at[q, d],
            device_id={"energy": mine * group + other},
            device_id_type=mesh_id,
        )

    def near_copy(side, q):
        return pltpu.make_async_remote_copy(
            src_ref=final_buf.at[q],
            dst_ref=near_buf.at[side, q],
            send_sem=near_send.at[side, q],
            recv_sem=near_recv.at[side, q],
            device_id={"space": lax.rem(row + (rows - 1 if side else 1), rows)},
            device_id_type=mesh_id,
        )

    def near_if(side, receiving, body, other=None):
        if rows == 2:
            body()
        else:
            there = row > 0 if bool(side) != receiving else row < rows - 1
            pl.when(there)(body)
            if other is not None:
                pl.when(jnp.logical_not(there))(other)

    def edge_copy():
        return pltpu.make_async_remote_copy(
            src_ref=upper,
            dst_ref=before_buf,
            send_sem=edge_sem.at[0],
            recv_sem=edge_sem.at[1],
            device_id={"space": lax.rem(row + 1, rows)},
            device_id_type=mesh_id,
        )

    def result_copy(item):
        return pltpu.make_async_copy(total_buf.at[item], out.at[item], result_sem.at[item])

    each(0, SLOTS, lambda u: raw_copy(u).start())
    barrier = pltpu.get_barrier_semaphore()
    each(1, n, lambda d: pl.semaphore_signal(
        barrier, inc=1, device_id={"energy": lax.rem(me + d, n)}, device_id_type=mesh_id))
    for side in range(sides):
        pl.semaphore_signal(
            barrier, inc=1, device_id={"space": lax.rem(row + (rows - 1 if side else 1), rows)}, device_id_type=mesh_id)
    pl.semaphore_wait(barrier, n - 1 + sides)

    def send_kind(k, q):
        in_own(k, q).start()
        each(1, group, lambda d: in_copy(k, q, d).start())

    def send_stage(q):
        for k in range(2):
            send_kind(k, q)

    def prepare():
        edge_copy().wait()
        before, above = before_buf[...], upper[...]
        if rows == 2:
            link = jnp.where(row == 0, above, before)
            turned = link.T
            couplings = [(jnp.where(row == 0, link, turned), jnp.where(row == 0, turned, link))]
        else:
            before = jnp.where(row > 0, before, 0.0)
            above = jnp.where(row < rows - 1, above, 0.0)
            couplings = [(before.T, before), (above, above.T)]
        pairs = [(diag[...], diag[...])] + couplings
        for side, (_, right) in enumerate(pairs):
            for half in range(width // LANES):
                right_tab[side, half] = stacked(right[half * LANES:(half + 1) * LANES])
        for part in range(parts):
            columns = slice(part * PART, (part + 1) * PART)
            left_tab[part] = jnp.concatenate([spread(left[:, columns]) for left, _ in pairs], axis=1)

    def forward_stage(q):
        for k in range(2):
            in_own(k, q).wait()
            each(1, group, lambda d: in_copy(k, q, d).wait_recv())

            @pl.when(halo_sends(k, q))
            def _():
                halo_copy(k, q).start()

    def pair(tile, i):
        return jnp.concatenate([tile[:, :, i + s].reshape(2 * keep, LANES) for s in range(2)], axis=1)

    def compute_stage(q):
        alone = mine == pivot(q)

        @pl.when(jnp.logical_not(alone))
        def _():
            halo_copy(0, q).wait_recv()

        @pl.when(alone)
        def _():
            halo_buf[q] = jnp.zeros(halo_buf.shape[1:], jnp.float32)

        @pl.when(slot_sent(q))
        def _():
            halo_copy(0, q).wait_send()

        wide = jnp.where(mine > pivot(q), 1, 0)
        slot = polar_slot(q)
        for i in range(0, ROWS, 2):
            own = pair(in_buf.at[wide, q], i)
            other = pair(in_buf.at[1 - wide, q], i)
            halo = pair(halo_buf.at[q], i)
            spec_a = dot(wide_tab[wide], jnp.concatenate([own, halo], axis=0))
            spec_b = dot(narrow_tab[1 - wide], other)
            mid = spec_a.shape[0] // 2
            ar, ai, br, bi = spec_a[:mid], spec_a[mid:], spec_b[:mid], spec_b[mid:]
            spec = jnp.concatenate([ar * br - ai * bi, ar * bi + ai * br], axis=0)
            polar = dot(back_tab[...], spec)
            for s in range(2):
                in_buf[slot, q, :, :, i + s] = polar[:, s * LANES:(s + 1) * LANES].reshape(2, keep, LANES)

    def chain_stage(up, q):
        far = 0 if up else last
        slot = polar_slot(q)

        def hop(j):
            @pl.when(mine != far)
            def _():
                chain_copy(up, q, j).wait_recv()
                here = pl.ds(j * block, block)
                in_buf[slot, q, :, here] = in_buf[slot, q, :, here] + chain_buf[q, j + up]

            @pl.when(mine != j)
            def _():
                chain_copy(up, q, j).start()

        if up:
            each(0, last - mine + 1, lambda t: hop(last - t))
        else:
            each(0, mine + 1, hop)

    def final_stage(q):
        final_buf[q, :, :, share] = in_buf[polar_slot(q), q, :, pl.ds(me * kept, kept)]
        each(1, group, lambda d: out_copy(q, d).start())

    def halfway(side, q, value):
        half, tile = q // tiles, lax.rem(q, tiles)
        term = product(spread(value.reshape(count * group * ROWS, LANES)), right_tab[side, half])
        half_buf[side, :, tile] = half_buf[side, :, tile] + term.reshape(count, group, ROWS, width)

    def near_stage(q):
        each(1, group, lambda d: out_copy(q, d).wait_recv())
        for side in range(sides):
            near_if(side, False, lambda: near_copy(side, q).start())
        halfway(0, q, final_buf[q])

    def screen_part(part):
        def one(item):
            terms = [
                stacked(half_buf[side, item, pl.ds(part * per_part, per_part)].reshape(PART, width))
                for side in range(1 + sides)
            ]
            total_buf[item] = total_buf[item] + product(left_tab[part], jnp.concatenate(terms, axis=0))

            @pl.when(part == parts - 1)
            def _():
                result_copy(item).start()

        each(0, count, one)

    def screen_stage(q):
        for side in range(sides):
            def arrived():
                near_copy(side, q).wait_recv()
                halfway(1 + side, q, near_buf[side, q])
            near_if(side, True, arrived)
        done = q + 1 - (stages - tiles)

        @pl.when(jnp.logical_and(done > 0, lax.rem(done, per_part) == 0))
        def _():
            screen_part(done // per_part - 1)

    def at(q, body):
        pl.when(jnp.logical_and(q >= 0, q < stages))(lambda: body(q))

    edge_copy().start()
    ahead = min(AHEAD, tiles)
    each(0, ahead, lambda q: send_kind(0, q))
    flip_half(0)
    each(0, ahead, lambda q: send_kind(1, q))
    for half in range(1, width // LANES):
        flip_half(half)
    half_buf[...] = jnp.zeros(half_buf.shape, jnp.float32)
    total_buf[...] = jnp.zeros(total_buf.shape, jnp.float32)
    prepare()
    below = last - mine
    late = jnp.maximum(mine, below)

    def step(i):
        at(i + ahead, send_stage)
        at(i, forward_stage)
        at(i - 1, compute_stage)
        at(i - 1 - mine, lambda q: chain_stage(1, q))
        at(i - 1 - below, lambda q: chain_stage(0, q))
        at(i - 1 - late, final_stage)
        at(i - 2 - late - ahead, near_stage)
        at(i - 3 - late - ahead, screen_stage)

    each(0, stages + 3 + last + ahead, step)

    def finish(q):
        for side in range(sides):
            near_if(side, False, lambda: near_copy(side, q).wait_send())
        for k in range(2):
            each(1, group, lambda d: in_copy(k, q, d).wait_send())

            @pl.when(jnp.logical_and(halo_sends(k, q), jnp.logical_not(slot_sent(q))) if k == 0 else halo_sends(k, q))
            def _():
                halo_copy(k, q).wait_send()
        each(mine + 1, groups, lambda j: chain_copy(1, q, j).wait_send())
        each(0, mine, lambda j: chain_copy(0, q, j).wait_send())
        each(1, group, lambda d: out_copy(q, d).wait_send())

    each(0, stages, finish)
    each(0, count, lambda item: result_copy(item).wait())


def local(g_lesser, g_greater, v_diag, v_upper):
    n, rows = lax.axis_size("energy"), lax.axis_size("space")
    sides = 1 if rows == 2 else 2
    _, held, _, size, width = g_lesser.shape
    keep = NW
    group = keep // held
    groups = n // group
    tiles = size // group // ROWS
    halves = width // LANES
    stages = tiles * halves
    kept = keep // n
    parts = size // PART
    less = g_lesser.reshape(2, held, tiles, group, ROWS, width)
    great = g_greater.reshape(2, held, size, width)
    tabs = tables(keep)
    vmem_spec = pl.BlockSpec(memory_space=pltpu.VMEM)
    any_spec = pl.BlockSpec(memory_space=pl.ANY)
    dma = pltpu.SemaphoreType.DMA

    def vmem(*dims, dtype=jnp.float32):
        return pltpu.VMEM(dims, dtype)

    def tiled(*dims):
        return vmem(*dims, ROWS, LANES)

    out = pl.pallas_call(
        functools.partial(screening_kernel, n, group, rows),
        out_shape=jax.ShapeDtypeStruct((2 * kept, size, width), jnp.float32),
        in_specs=[vmem_spec] * (len(tabs) + 2) + [any_spec] * 2,
        out_specs=any_spec,
        scratch_shapes=[
            vmem(SLOTS, LANES, width),
            tiled(halves, 2, held, tiles, group),
            tiled(2, stages, 2, keep),
            tiled(stages, 2, keep),
            tiled(stages, groups + 1, 2, group * kept),
            tiled(stages, 2, kept, group),
            tiled(sides, stages, 2, kept, group),
            vmem(1 + sides, 2 * kept, tiles, group, ROWS, width),
            vmem(2 * kept, size, width),
            vmem(size, width),
            vmem(1 + sides, halves, 3 * LANES, width, dtype=jnp.bfloat16),
            vmem(parts, size, 3 * PART * (1 + sides), dtype=jnp.bfloat16),
            dma((SLOTS,)),
            dma((2, stages, group)), dma((2, stages, group)), dma((2, stages)),
            dma((2, stages)), dma((stages,)),
            dma((2, stages, groups)), dma((2, stages, groups)),
            dma((stages, group)), dma((stages, group)),
            dma((sides, stages)), dma((sides, stages)),
            dma((2,)), dma((2 * kept,)),
        ],
        compiler_params=pltpu.CompilerParams(
            collective_id=0, has_side_effects=True, vmem_limit_bytes=2**26 - 2**16),
    )(*tabs, v_diag[0], v_upper[0], less, great)
    return out.reshape(2, kept, 1, size, width)


def solution(mesh):
    in_specs = (
        P(None, "energy", "space", None, None),
        P(None, "energy", "space", None, None),
        P("space", None, None),
        P("space", None, None),
    )
    out_specs = P(None, "energy", "space", None, None)
    return jax.shard_map(local, mesh=mesh, in_specs=in_specs, out_specs=out_specs, check_vma=False)
```

```python
import functools
import math

import jax
import jax.numpy as jnp
import numpy as np
from jax import lax
from jax.experimental import pallas as pl
from jax.experimental.pallas import tpu as pltpu
from jax.sharding import PartitionSpec as P

NW = 64
PREFACTOR = 0.0625
ROWS = 8
LANES = 128
AHEAD = 3
FIRST = 4
EARLY = 12
READY = 3
HOP = 4
TURN = 4
NEAR = 3
SCREEN = 4
CORES = 2
PART = 64
SLOTS = 4


def split_np(table):
    table = np.asarray(table, np.float64)
    high = table.astype(jnp.bfloat16)
    low = (table - high.astype(np.float64)).astype(jnp.bfloat16)
    return np.concatenate([high, low, high], axis=1)


def tables(keep):
    length = 2 * keep

    def forward(start, sign):
        phase = 2.0 * math.pi / length * (np.outer(np.arange(length), np.arange(start, start + keep)) % length)
        cos, sin = np.cos(phase), sign * np.sin(phase)
        return np.block([[cos, sin], [-sin, cos]])

    phase = 2.0 * math.pi / length * (np.outer(np.arange(keep), np.arange(length)) % length)
    cos, sin = np.cos(phase) * (PREFACTOR / length), np.sin(phase) * (PREFACTOR / length)
    back = np.block([[cos, -sin], [sin, cos]])
    wide = [np.concatenate([forward(0, sign), forward(keep, sign)], axis=1) for sign in (1, -1)]
    narrow = [forward(0, sign) for sign in (1, -1)]
    return [jnp.asarray(t) for t in (
        np.stack([split_np(t) for t in wide]), np.stack([split_np(t) for t in narrow]), split_np(back))]


def split(value):
    high = value.astype(jnp.bfloat16)
    return high, (value - high.astype(jnp.float32)).astype(jnp.bfloat16)


def stacked(value):
    high, low = split(value)
    return jnp.concatenate([high, high, low], axis=0)


def spread(value):
    high, low = split(value)
    return jnp.concatenate([high, low, high], axis=1)


def product(left, right):
    return jnp.dot(left, right, preferred_element_type=jnp.float32)


def dot(table, value):
    return product(table, stacked(value))


def screening_kernel(
    n, group, rows, wide_tab, narrow_tab, back_tab, diag, upper, less, great, out,
    raw_buf, flip_buf, in_buf, halo_buf, chain_buf, final_buf, near_buf, half_buf, total_buf,
    before_buf, right_tab, left_tab,
    raw_sem, in_send, in_recv, own_sem, mate_send, mate_recv, halo_send, halo_recv, chain_send, chain_recv,
    out_send, out_recv, close_send, close_recv, near_send, near_recv, edge_sem, result_sem,
):
    me = lax.axis_index("energy")
    mine, share = me // group, lax.rem(me, group)
    groups = n // group
    last = groups - 1
    row = lax.axis_index("space")
    held, size, width = great.shape[1:]
    tiles = less.shape[2]
    sides = near_buf.shape[0]
    stages = in_buf.shape[1]
    keep = in_buf.shape[3]
    count = out.shape[0]
    kept = count // 2
    block = group * kept
    parts = left_tab.shape[0]
    per_part = tiles // parts
    cores = mate_recv.shape[1]
    chip, core, chips = share // cores, lax.rem(share, cores), group // cores
    mesh_id = pl.DeviceIdType.MESH

    def each(first, last, body):
        def step(d, carry):
            body(d)
            return carry
        lax.fori_loop(first, last, step, 0)

    def raw_copy(u):
        half, rest = u // (2 * held), lax.rem(u, 2 * held)
        slot = lax.rem(u, SLOTS)
        return pltpu.make_async_copy(
            great.at[rest // held, lax.rem(rest, held), pl.ds(pl.multiple_of(half * LANES, LANES), LANES)],
            raw_buf.at[slot], raw_sem.at[slot])

    def flip_half(half):
        first = half * 2 * held

        def flip(r):
            u = first + r
            raw_copy(u).wait()
            flip_buf[half, r // held, lax.rem(r, held)] = raw_buf[lax.rem(u, SLOTS)].T.reshape(
                tiles, group, ROWS, LANES)

            @pl.when(u + SLOTS < 2 * held * (width // LANES))
            def _():
                raw_copy(u + SLOTS).start()

        each(0, 2 * held, flip)

    def source(k, q, other):
        half, tile = q // tiles, lax.rem(q, tiles)
        if k:
            return flip_buf.at[half, :, :, tile, other]
        return less.at[:, :, tile, other, :, pl.ds(pl.multiple_of(half * LANES, LANES), LANES)]

    def in_copy(k, q, d):
        other = lax.rem(share + d, group)
        return pltpu.make_async_remote_copy(
            src_ref=source(k, q, other),
            dst_ref=in_buf.at[k, q, :, pl.ds(share * held, held)],
            send_sem=in_send.at[k, q, d],
            recv_sem=in_recv.at[k, q, d],
            device_id={"energy": mine * group + other},
            device_id_type=mesh_id,
        )

    def in_own(k, q):
        return pltpu.make_async_copy(
            source(k, q, share), in_buf.at[k, q, :, pl.ds(share * held, held)], own_sem.at[k, q])

    def pivot(q):
        outer = q * ((groups + 1) // 2) // stages
        return jnp.where(lax.rem(q, 2) == 0, outer, last - outer)

    def beside(k):
        return lax.rem(mine + (1 if k else groups - 1), groups)

    def mate_copy(k, q, c):
        there = chip * cores + c
        return pltpu.make_async_remote_copy(
            src_ref=source(k, q, there),
            dst_ref=halo_buf.at[q, :, pl.ds(share * held, held)],
            send_sem=mate_send.at[k, q, c],
            recv_sem=mate_recv.at[q, core],
            device_id={"energy": beside(k) * group + there},
            device_id_type=mesh_id,
        )

    def mate_wait(q, c):
        pltpu.make_async_remote_copy(
            src_ref=source(0, q, share),
            dst_ref=halo_buf.at[q, :, pl.ds((chip * cores + c) * held, held)],
            send_sem=mate_send.at[0, q, c],
            recv_sem=mate_recv.at[q, c],
            device_id={"energy": beside(0) * group + share},
            device_id_type=mesh_id,
        ).wait_recv()

    def halo_copy(k, q, d):
        energies = pl.ds(lax.rem(chip + d, chips) * cores * held, cores * held)
        return pltpu.make_async_remote_copy(
            src_ref=in_buf.at[k, q, :, energies],
            dst_ref=halo_buf.at[q, :, energies],
            send_sem=halo_send.at[k, q, d],
            recv_sem=halo_recv.at[q, d],
            device_id={"energy": beside(k) * group + share},
            device_id_type=mesh_id,
        )

    def halo_sends(k, q):
        if k:
            return jnp.logical_and(mine >= pivot(q), mine < last)
        return jnp.logical_and(mine <= pivot(q), mine > 0)

    def polar_slot(q):
        return jnp.where(jnp.logical_or(mine < pivot(q), mine == last), 1, 0)

    def slot_sent(q):
        return jnp.logical_and(mine == pivot(q), jnp.logical_and(mine > 0, mine < last))

    def chain_copy(up, q, j):
        peer = lax.rem(me + (group if up else n - group), n)
        return pltpu.make_async_remote_copy(
            src_ref=in_buf.at[polar_slot(q), q, :, pl.ds(j * block, block)],
            dst_ref=chain_buf.at[q, j + up],
            send_sem=chain_send.at[up, q, j],
            recv_sem=chain_recv.at[up, q, j],
            device_id={"energy": peer},
            device_id_type=mesh_id,
        )

    def out_copy(q, d):
        other = lax.rem(share + d, group)
        return pltpu.make_async_remote_copy(
            src_ref=in_buf.at[polar_slot(q), q, :, pl.ds((mine * group + other) * kept, kept)],
            dst_ref=final_buf.at[q, :, :, share],
            send_sem=out_send.at[q, d],
            recv_sem=out_recv.at[q, d],
            device_id={"energy": mine * group + other},
            device_id_type=mesh_id,
        )

    def row_of(side):
        return lax.rem(row + (rows - 1 if side else 1), rows)

    def close_copy(side, q, c):
        there = mine * group + chip * cores + c
        return pltpu.make_async_remote_copy(
            src_ref=in_buf.at[polar_slot(q), q, :, pl.ds(there * kept, kept)],
            dst_ref=near_buf.at[side, q, :, :, share],
            send_sem=close_send.at[side, q, c],
            recv_sem=close_recv.at[side, q, core],
            device_id={"energy": there, "space": row_of(side)},
            device_id_type=mesh_id,
        )

    def close_wait(side, q, c):
        pltpu.make_async_remote_copy(
            src_ref=in_buf.at[0, q, :, pl.ds(0, kept)],
            dst_ref=near_buf.at[side, q, :, :, chip * cores + c],
            send_sem=close_send.at[side, q, c],
            recv_sem=close_recv.at[side, q, c],
            device_id={"space": row_of(side)},
            device_id_type=mesh_id,
        ).wait_recv()

    def near_copy(side, q, d):
        shares = pl.ds(lax.rem(chip + d, chips) * cores, cores)
        return pltpu.make_async_remote_copy(
            src_ref=final_buf.at[q, :, :, shares],
            dst_ref=near_buf.at[side, q, :, :, shares],
            send_sem=near_send.at[side, q, d],
            recv_sem=near_recv.at[side, q, d],
            device_id={"space": row_of(side)},
            device_id_type=mesh_id,
        )

    def near_if(side, receiving, body, other=None):
        if rows == 2:
            body()
        else:
            there = row > 0 if bool(side) != receiving else row < rows - 1
            pl.when(there)(body)
            if other is not None:
                pl.when(jnp.logical_not(there))(other)

    def edge_copy():
        return pltpu.make_async_remote_copy(
            src_ref=upper,
            dst_ref=before_buf,
            send_sem=edge_sem.at[0],
            recv_sem=edge_sem.at[1],
            device_id={"space": lax.rem(row + 1, rows)},
            device_id_type=mesh_id,
        )

    def result_copy(item):
        return pltpu.make_async_copy(total_buf.at[item], out.at[item], result_sem.at[item])

    each(0, SLOTS, lambda u: raw_copy(u).start())
    barrier = pltpu.get_barrier_semaphore()
    each(1, n, lambda d: pl.semaphore_signal(
        barrier, inc=1, device_id={"energy": lax.rem(me + d, n)}, device_id_type=mesh_id))
    for side in range(sides):
        each(0, cores, lambda c: pl.semaphore_signal(
            barrier, inc=1, device_id={"energy": mine * group + chip * cores + c, "space": row_of(side)},
            device_id_type=mesh_id))
    pl.semaphore_wait(barrier, n - 1 + sides * cores)

    def send_kind(k, q):
        in_own(k, q).start()
        each(1, group, lambda d: in_copy(k, q, d).start())

    def mate_kind(k, q):
        @pl.when(halo_sends(k, q))
        def _():
            each(0, cores, lambda c: mate_copy(k, q, c).start())

    def prepare():
        edge_copy().wait()
        before, above = before_buf[...], upper[...]
        if rows == 2:
            link = jnp.where(row == 0, above, before)
            turned = link.T
            couplings = [(jnp.where(row == 0, link, turned), jnp.where(row == 0, turned, link))]
        else:
            before = jnp.where(row > 0, before, 0.0)
            above = jnp.where(row < rows - 1, above, 0.0)
            couplings = [(before.T, before), (above, above.T)]
        pairs = [(diag[...], diag[...])] + couplings
        for side, (_, right) in enumerate(pairs):
            for half in range(width // LANES):
                right_tab[side, half] = stacked(right[half * LANES:(half + 1) * LANES])
        for part in range(parts):
            columns = slice(part * PART, (part + 1) * PART)
            left_tab[part] = jnp.concatenate([spread(left[:, columns]) for left, _ in pairs], axis=1)

    def forward_kind(k, q):
        in_own(k, q).wait()
        each(1, group, lambda d: in_copy(k, q, d).wait_recv())

        @pl.when(halo_sends(k, q))
        def _():
            each(1, chips, lambda d: halo_copy(k, q, d).start())

    def pair(tile, i):
        return jnp.concatenate([tile[:, :, i + s].reshape(2 * keep, LANES) for s in range(2)], axis=1)

    def compute_stage(q):
        alone = mine == pivot(q)

        @pl.when(jnp.logical_not(alone))
        def _():
            each(0, cores, lambda c: mate_wait(q, c))
            each(1, chips, lambda d: halo_copy(0, q, d).wait_recv())

        @pl.when(alone)
        def _():
            halo_buf[q] = jnp.zeros(halo_buf.shape[1:], jnp.float32)

        @pl.when(slot_sent(q))
        def _():
            each(1, chips, lambda d: halo_copy(0, q, d).wait_send())

        wide = jnp.where(mine > pivot(q), 1, 0)
        slot = polar_slot(q)
        for i in range(0, ROWS, 2):
            own = pair(in_buf.at[wide, q], i)
            other = pair(in_buf.at[1 - wide, q], i)
            halo = pair(halo_buf.at[q], i)
            spec_a = dot(wide_tab[wide], jnp.concatenate([own, halo], axis=0))
            spec_b = dot(narrow_tab[1 - wide], other)
            mid = spec_a.shape[0] // 2
            ar, ai, br, bi = spec_a[:mid], spec_a[mid:], spec_b[:mid], spec_b[mid:]
            spec = jnp.concatenate([ar * br - ai * bi, ar * bi + ai * br], axis=0)
            polar = dot(back_tab[...], spec)
            for s in range(2):
                in_buf[slot, q, :, :, i + s] = polar[:, s * LANES:(s + 1) * LANES].reshape(2, keep, LANES)

    def chain_stage(up, q):
        far = 0 if up else last
        slot = polar_slot(q)

        def hop(j):
            @pl.when(mine != far)
            def _():
                chain_copy(up, q, j).wait_recv()
                here = pl.ds(j * block, block)
                in_buf[slot, q, :, here] = in_buf[slot, q, :, here] + chain_buf[q, j + up]

            @pl.when(mine != j)
            def _():
                chain_copy(up, q, j).start()

        if up:
            each(0, last - mine + 1, lambda t: hop(last - t))
        else:
            each(0, mine + 1, hop)

    def final_stage(q):
        final_buf[q, :, :, share] = in_buf[polar_slot(q), q, :, pl.ds(me * kept, kept)]
        for side in range(sides):
            near_if(side, False, lambda: each(0, cores, lambda c: close_copy(side, q, c).start()))

    def out_stage(q):
        each(1, group, lambda d: out_copy(q, d).start())

    def halfway(side, q, value):
        half, tile = q // tiles, lax.rem(q, tiles)
        term = product(spread(value.reshape(count * group * ROWS, LANES)), right_tab[side, half])
        half_buf[side, :, tile] = half_buf[side, :, tile] + term.reshape(count, group, ROWS, width)

    def near_stage(q):
        each(1, group, lambda d: out_copy(q, d).wait_recv())
        for side in range(sides):
            near_if(side, False, lambda: each(1, chips, lambda d: near_copy(side, q, d).start()))
        halfway(0, q, final_buf[q])

    def screen_part(part):
        def one(item):
            terms = [
                stacked(half_buf[side, item, pl.ds(part * per_part, per_part)].reshape(PART, width))
                for side in range(1 + sides)
            ]
            total_buf[item] = total_buf[item] + product(left_tab[part], jnp.concatenate(terms, axis=0))

            @pl.when(part == parts - 1)
            def _():
                result_copy(item).start()

        each(0, count, one)

    def screen_stage(q):
        for side in range(sides):
            def arrived():
                each(0, cores, lambda c: close_wait(side, q, c))
                each(1, chips, lambda d: near_copy(side, q, d).wait_recv())
                halfway(1 + side, q, near_buf[side, q])
            near_if(side, True, arrived)
        done = q + 1 - (stages - tiles)

        @pl.when(jnp.logical_and(done > 0, lax.rem(done, per_part) == 0))
        def _():
            screen_part(done // per_part - 1)

    def by_kind(v, begin, body):
        for k in range(2):
            @pl.when(jnp.logical_and(lax.rem(v, 2) == k, jnp.logical_and(v >= begin, v < 2 * stages)))
            def _():
                body(k, v // 2)

    def at(v, body):
        ready = jnp.logical_and(v >= 0, v < 2 * stages)
        pl.when(jnp.logical_and(ready, lax.rem(v, 2) == 0))(lambda: body(v // 2))

    def clear():
        half_buf[...] = jnp.zeros(half_buf.shape, jnp.float32)
        total_buf[...] = jnp.zeros(total_buf.shape, jnp.float32)

    first, early = min(FIRST, 2 * tiles), min(EARLY, 2 * tiles)
    send_kind(0, 0)
    each(0, early // 2, lambda q: mate_kind(0, q))
    edge_copy().start()
    flip_half(0)
    each(1, first, lambda v: by_kind(v, 1, send_kind))
    each(0, early // 2, lambda q: mate_kind(1, q))
    clear()
    below = last - mine
    settled = READY + HOP * jnp.maximum(mine, below)
    turn = max(2 * stages - TURN, 0)

    def turned(v, body):
        steady = v >= 2 * turn - settled
        q = jnp.where(steady, (v - settled) // 2, v - turn)
        begun = jnp.where(steady, jnp.where(v >= settled, lax.rem(v - settled, 2) == 0, False), v >= turn)
        pl.when(jnp.logical_and(begun, q < stages))(lambda: body(q))

    def step(u):
        by_kind(u + AHEAD, first, send_kind)
        by_kind(u + early, early, mate_kind)
        by_kind(u, 0, forward_kind)
        for half in range(1, width // LANES):
            pl.when(u == 0)(lambda: flip_half(half))
        pl.when(u == 1)(prepare)
        at(u - READY, compute_stage)
        at(u - READY - HOP * mine, lambda q: chain_stage(1, q))
        at(u - READY - HOP * below, lambda q: chain_stage(0, q))
        at(u - settled, final_stage)
        turned(u, out_stage)
        turned(u - NEAR, near_stage)
        turned(u - NEAR - SCREEN, screen_stage)

    length = max(2 * stages - 1 + READY + HOP * last, turn + stages)
    each(0, length + NEAR + SCREEN, step)

    def finish(q):
        for side in range(sides):
            near_if(side, False, lambda: each(0, cores, lambda c: close_copy(side, q, c).wait_send()))
            near_if(side, False, lambda: each(1, chips, lambda d: near_copy(side, q, d).wait_send()))
        for k in range(2):
            each(1, group, lambda d: in_copy(k, q, d).wait_send())

            @pl.when(jnp.logical_and(halo_sends(k, q), jnp.logical_not(slot_sent(q))) if k == 0 else halo_sends(k, q))
            def _():
                each(1, chips, lambda d: halo_copy(k, q, d).wait_send())

            @pl.when(halo_sends(k, q))
            def _():
                each(0, cores, lambda c: mate_copy(k, q, c).wait_send())
        each(mine + 1, groups, lambda j: chain_copy(1, q, j).wait_send())
        each(0, mine, lambda j: chain_copy(0, q, j).wait_send())
        each(1, group, lambda d: out_copy(q, d).wait_send())

    each(0, stages, finish)
    each(0, count, lambda item: result_copy(item).wait())


def local(g_lesser, g_greater, v_diag, v_upper):
    n, rows = lax.axis_size("energy"), lax.axis_size("space")
    sides = 1 if rows == 2 else 2
    _, held, _, size, width = g_lesser.shape
    keep = NW
    group = keep // held
    groups = n // group
    tiles = size // group // ROWS
    halves = width // LANES
    stages = tiles * halves
    kept = keep // n
    parts = size // PART
    cores = CORES if group % CORES == 0 else 1
    less = g_lesser.reshape(2, held, tiles, group, ROWS, width)
    great = g_greater.reshape(2, held, size, width)
    tabs = tables(keep)
    vmem_spec = pl.BlockSpec(memory_space=pltpu.VMEM)
    any_spec = pl.BlockSpec(memory_space=pl.ANY)
    dma = pltpu.SemaphoreType.DMA

    def vmem(*dims, dtype=jnp.float32):
        return pltpu.VMEM(dims, dtype)

    def tiled(*dims):
        return vmem(*dims, ROWS, LANES)

    out = pl.pallas_call(
        functools.partial(screening_kernel, n, group, rows),
        out_shape=jax.ShapeDtypeStruct((2 * kept, size, width), jnp.float32),
        in_specs=[vmem_spec] * (len(tabs) + 2) + [any_spec] * 2,
        out_specs=any_spec,
        scratch_shapes=[
            vmem(SLOTS, LANES, width),
            tiled(halves, 2, held, tiles, group),
            tiled(2, stages, 2, keep),
            tiled(stages, 2, keep),
            tiled(stages, groups + 1, 2, group * kept),
            tiled(stages, 2, kept, group),
            tiled(sides, stages, 2, kept, group),
            vmem(1 + sides, 2 * kept, tiles, group, ROWS, width),
            vmem(2 * kept, size, width),
            vmem(size, width),
            vmem(1 + sides, halves, 3 * LANES, width, dtype=jnp.bfloat16),
            vmem(parts, size, 3 * PART * (1 + sides), dtype=jnp.bfloat16),
            dma((SLOTS,)),
            dma((2, stages, group)), dma((2, stages, group)), dma((2, stages)),
            dma((2, stages, cores)), dma((stages, cores)),
            dma((2, stages, group // cores)), dma((stages, group // cores)),
            dma((2, stages, groups)), dma((2, stages, groups)),
            dma((stages, group)), dma((stages, group)),
            dma((sides, stages, cores)), dma((sides, stages, cores)),
            dma((sides, stages, group // cores)), dma((sides, stages, group // cores)),
            dma((2,)), dma((2 * kept,)),
        ],
        compiler_params=pltpu.CompilerParams(
            collective_id=0, has_side_effects=True, vmem_limit_bytes=2**26 - 2**16),
    )(*tabs, v_diag[0], v_upper[0], less, great)
    return out.reshape(2, kept, 1, size, width)


def solution(mesh):
    in_specs = (
        P(None, "energy", "space", None, None),
        P(None, "energy", "space", None, None),
        P("space", None, None),
        P("space", None, None),
    )
    out_specs = P(None, "energy", "space", None, None)
    return jax.shard_map(local, mesh=mesh, in_specs=in_specs, out_specs=out_specs, check_vma=False)
```

```python
import functools
import math

import jax
import jax.numpy as jnp
import numpy as np
from jax import lax
from jax.experimental import pallas as pl
from jax.experimental.pallas import tpu as pltpu
from jax.sharding import PartitionSpec as P

NW = 64
PREFACTOR = 0.0625
ROWS = 8
LANES = 128
AHEAD = 3
FIRST = 4
EARLY = 12
HOP = 3
TURN = 4
BURST = 3
QUICK = 0
NEAR = 4
SCREEN = 6
CORES = 2
PART = 64
SLOTS = 4


def split_np(table):
    table = np.asarray(table, np.float64)
    high = table.astype(jnp.bfloat16)
    low = (table - high.astype(np.float64)).astype(jnp.bfloat16)
    return np.concatenate([high, low, high], axis=1)


def tables(keep):
    length = 2 * keep

    def forward(start, sign):
        phase = 2.0 * math.pi / length * (np.outer(np.arange(length), np.arange(start, start + keep)) % length)
        cos, sin = np.cos(phase), sign * np.sin(phase)
        return np.block([[cos, sin], [-sin, cos]])

    phase = 2.0 * math.pi / length * (np.outer(np.arange(keep), np.arange(length)) % length)
    cos, sin = np.cos(phase) * (PREFACTOR / length), np.sin(phase) * (PREFACTOR / length)
    back = np.block([[cos, -sin], [sin, cos]])
    wide = [np.concatenate([forward(0, sign), forward(keep, sign)], axis=1) for sign in (1, -1)]
    narrow = [forward(0, sign) for sign in (1, -1)]
    return [jnp.asarray(t) for t in (
        np.stack([split_np(t) for t in wide]), np.stack([split_np(t) for t in narrow]), split_np(back))]


def split(value):
    high = value.astype(jnp.bfloat16)
    return high, (value - high.astype(jnp.float32)).astype(jnp.bfloat16)


def stacked(value):
    high, low = split(value)
    return jnp.concatenate([high, high, low], axis=0)


def spread(value):
    high, low = split(value)
    return jnp.concatenate([high, low, high], axis=1)


def product(left, right):
    return jnp.dot(left, right, preferred_element_type=jnp.float32)


def dot(table, value):
    return product(table, stacked(value))


def screening_kernel(
    n, group, rows, wide_tab, narrow_tab, back_tab, diag, upper, less, great, out,
    raw_buf, flip_buf, in_buf, halo_buf, chain_buf, final_buf, near_buf, half_buf, total_buf,
    before_buf, right_tab, left_tab,
    raw_sem, in_send, in_recv, own_sem, mate_send, mate_recv, halo_send, halo_recv, chain_send, chain_recv,
    out_send, out_recv, close_send, close_recv, near_send, near_recv, edge_sem, result_sem,
):
    me = lax.axis_index("energy")
    mine, share = me // group, lax.rem(me, group)
    groups = n // group
    last = groups - 1
    row = lax.axis_index("space")
    held, size, width = great.shape[1:]
    tiles = less.shape[2]
    sides = near_buf.shape[0]
    stages = in_buf.shape[1]
    keep = in_buf.shape[3]
    count = out.shape[0]
    kept = count // 2
    block = group * kept
    parts = left_tab.shape[0]
    per_part = tiles // parts
    cores = mate_recv.shape[1]
    chip, core, chips = share // cores, lax.rem(share, cores), group // cores
    mesh_id = pl.DeviceIdType.MESH

    def each(first, last, body):
        def step(d, carry):
            body(d)
            return carry
        lax.fori_loop(first, last, step, 0)

    def raw_copy(u):
        half, rest = u // (2 * held), lax.rem(u, 2 * held)
        slot = lax.rem(u, SLOTS)
        return pltpu.make_async_copy(
            great.at[rest // held, lax.rem(rest, held), pl.ds(pl.multiple_of(half * LANES, LANES), LANES)],
            raw_buf.at[slot], raw_sem.at[slot])

    def flip_half(half):
        first = half * 2 * held

        def flip(r):
            u = first + r
            raw_copy(u).wait()
            flip_buf[half, r // held, lax.rem(r, held)] = raw_buf[lax.rem(u, SLOTS)].T.reshape(
                tiles, group, ROWS, LANES)

            @pl.when(u + SLOTS < 2 * held * (width // LANES))
            def _():
                raw_copy(u + SLOTS).start()

        each(0, 2 * held, flip)

    def source(k, q, other):
        half, tile = q // tiles, lax.rem(q, tiles)
        if k:
            return flip_buf.at[half, :, :, tile, other]
        return less.at[:, :, tile, other, :, pl.ds(pl.multiple_of(half * LANES, LANES), LANES)]

    def in_copy(k, q, d):
        other = lax.rem(share + d, group)
        return pltpu.make_async_remote_copy(
            src_ref=source(k, q, other),
            dst_ref=in_buf.at[k, q, :, pl.ds(share * held, held)],
            send_sem=in_send.at[k, q, d],
            recv_sem=in_recv.at[k, q, d],
            device_id={"energy": mine * group + other},
            device_id_type=mesh_id,
        )

    def in_own(k, q):
        return pltpu.make_async_copy(
            source(k, q, share), in_buf.at[k, q, :, pl.ds(share * held, held)], own_sem.at[k, q])

    def pivot(q):
        outer = q * ((groups + 1) // 2) // stages
        return jnp.where(lax.rem(q, 2) == 0, outer, last - outer)

    def beside(k):
        return lax.rem(mine + (1 if k else groups - 1), groups)

    def mate_copy(k, q, c):
        there = chip * cores + c
        return pltpu.make_async_remote_copy(
            src_ref=source(k, q, there),
            dst_ref=halo_buf.at[q, :, pl.ds(share * held, held)],
            send_sem=mate_send.at[k, q, c],
            recv_sem=mate_recv.at[q, core],
            device_id={"energy": beside(k) * group + there},
            device_id_type=mesh_id,
        )

    def mate_wait(q, c):
        pltpu.make_async_remote_copy(
            src_ref=source(0, q, share),
            dst_ref=halo_buf.at[q, :, pl.ds((chip * cores + c) * held, held)],
            send_sem=mate_send.at[0, q, c],
            recv_sem=mate_recv.at[q, c],
            device_id={"energy": beside(0) * group + share},
            device_id_type=mesh_id,
        ).wait_recv()

    def halo_copy(k, q, d):
        energies = pl.ds(lax.rem(chip + d, chips) * cores * held, cores * held)
        return pltpu.make_async_remote_copy(
            src_ref=in_buf.at[k, q, :, energies],
            dst_ref=halo_buf.at[q, :, energies],
            send_sem=halo_send.at[k, q, d],
            recv_sem=halo_recv.at[q, d],
            device_id={"energy": beside(k) * group + share},
            device_id_type=mesh_id,
        )

    def halo_sends(k, q):
        if k:
            return jnp.logical_and(mine >= pivot(q), mine < last)
        return jnp.logical_and(mine <= pivot(q), mine > 0)

    def polar_slot(q):
        return jnp.where(jnp.logical_or(mine < pivot(q), mine == last), 1, 0)

    def slot_sent(q):
        return jnp.logical_and(mine == pivot(q), jnp.logical_and(mine > 0, mine < last))

    def chain_copy(up, q, j):
        peer = lax.rem(me + (group if up else n - group), n)
        return pltpu.make_async_remote_copy(
            src_ref=in_buf.at[polar_slot(q), q, :, pl.ds(j * block, block)],
            dst_ref=chain_buf.at[q, j + up],
            send_sem=chain_send.at[up, q, j],
            recv_sem=chain_recv.at[up, q, j],
            device_id={"energy": peer},
            device_id_type=mesh_id,
        )

    def out_copy(q, d):
        other = lax.rem(share + d, group)
        return pltpu.make_async_remote_copy(
            src_ref=in_buf.at[polar_slot(q), q, :, pl.ds((mine * group + other) * kept, kept)],
            dst_ref=final_buf.at[q, :, :, share],
            send_sem=out_send.at[q, d],
            recv_sem=out_recv.at[q, d],
            device_id={"energy": mine * group + other},
            device_id_type=mesh_id,
        )

    def row_of(side):
        return lax.rem(row + (rows - 1 if side else 1), rows)

    def close_copy(side, q, c):
        there = mine * group + chip * cores + c
        return pltpu.make_async_remote_copy(
            src_ref=in_buf.at[polar_slot(q), q, :, pl.ds(there * kept, kept)],
            dst_ref=near_buf.at[side, q, :, :, share],
            send_sem=close_send.at[side, q, c],
            recv_sem=close_recv.at[side, q, core],
            device_id={"energy": there, "space": row_of(side)},
            device_id_type=mesh_id,
        )

    def close_wait(side, q, c):
        pltpu.make_async_remote_copy(
            src_ref=in_buf.at[0, q, :, pl.ds(0, kept)],
            dst_ref=near_buf.at[side, q, :, :, chip * cores + c],
            send_sem=close_send.at[side, q, c],
            recv_sem=close_recv.at[side, q, c],
            device_id={"space": row_of(side)},
            device_id_type=mesh_id,
        ).wait_recv()

    def near_copy(side, q, d):
        shares = pl.ds(lax.rem(chip + d, chips) * cores, cores)
        return pltpu.make_async_remote_copy(
            src_ref=final_buf.at[q, :, :, shares],
            dst_ref=near_buf.at[side, q, :, :, shares],
            send_sem=near_send.at[side, q, d],
            recv_sem=near_recv.at[side, q, d],
            device_id={"space": row_of(side)},
            device_id_type=mesh_id,
        )

    def near_if(side, receiving, body, other=None):
        if rows == 2:
            body()
        else:
            there = row > 0 if bool(side) != receiving else row < rows - 1
            pl.when(there)(body)
            if other is not None:
                pl.when(jnp.logical_not(there))(other)

    def edge_copy():
        return pltpu.make_async_remote_copy(
            src_ref=upper,
            dst_ref=before_buf,
            send_sem=edge_sem.at[0],
            recv_sem=edge_sem.at[1],
            device_id={"space": lax.rem(row + 1, rows)},
            device_id_type=mesh_id,
        )

    def result_copy(item):
        return pltpu.make_async_copy(total_buf.at[item], out.at[item], result_sem.at[item])

    each(0, SLOTS, lambda u: raw_copy(u).start())
    barrier = pltpu.get_barrier_semaphore()
    each(1, n, lambda d: pl.semaphore_signal(
        barrier, inc=1, device_id={"energy": lax.rem(me + d, n)}, device_id_type=mesh_id))
    for side in range(sides):
        each(0, cores, lambda c: pl.semaphore_signal(
            barrier, inc=1, device_id={"energy": mine * group + chip * cores + c, "space": row_of(side)},
            device_id_type=mesh_id))
    pl.semaphore_wait(barrier, n - 1 + sides * cores)

    def send_kind(k, q):
        in_own(k, q).start()
        each(1, group, lambda d: in_copy(k, q, d).start())

    def mate_kind(k, q):
        @pl.when(halo_sends(k, q))
        def _():
            each(0, cores, lambda c: mate_copy(k, q, c).start())

    def prepare():
        edge_copy().wait()
        before, above = before_buf[...], upper[...]
        if rows == 2:
            link = jnp.where(row == 0, above, before)
            turned = link.T
            couplings = [(jnp.where(row == 0, link, turned), jnp.where(row == 0, turned, link))]
        else:
            before = jnp.where(row > 0, before, 0.0)
            above = jnp.where(row < rows - 1, above, 0.0)
            couplings = [(before.T, before), (above, above.T)]
        pairs = [(diag[...], diag[...])] + couplings
        for side, (_, right) in enumerate(pairs):
            for half in range(width // LANES):
                right_tab[side, half] = stacked(right[half * LANES:(half + 1) * LANES])
        for part in range(parts):
            columns = slice(part * PART, (part + 1) * PART)
            left_tab[part] = jnp.concatenate([spread(left[:, columns]) for left, _ in pairs], axis=1)

    def forward_kind(k, q):
        in_own(k, q).wait()
        each(1, group, lambda d: in_copy(k, q, d).wait_recv())

        @pl.when(halo_sends(k, q))
        def _():
            each(1, chips, lambda d: halo_copy(k, q, d).start())

    def pair(tile, i):
        return jnp.concatenate([tile[:, :, i + s].reshape(2 * keep, LANES) for s in range(2)], axis=1)

    def compute_stage(q):
        alone = mine == pivot(q)

        @pl.when(jnp.logical_not(alone))
        def _():
            each(0, cores, lambda c: mate_wait(q, c))
            each(1, chips, lambda d: halo_copy(0, q, d).wait_recv())

        @pl.when(alone)
        def _():
            halo_buf[q] = jnp.zeros(halo_buf.shape[1:], jnp.float32)

        @pl.when(slot_sent(q))
        def _():
            each(1, chips, lambda d: halo_copy(0, q, d).wait_send())

        wide = jnp.where(mine > pivot(q), 1, 0)
        slot = polar_slot(q)
        for i in range(0, ROWS, 2):
            own = pair(in_buf.at[wide, q], i)
            other = pair(in_buf.at[1 - wide, q], i)
            halo = pair(halo_buf.at[q], i)
            spec_a = dot(wide_tab[wide], jnp.concatenate([own, halo], axis=0))
            spec_b = dot(narrow_tab[1 - wide], other)
            mid = spec_a.shape[0] // 2
            ar, ai, br, bi = spec_a[:mid], spec_a[mid:], spec_b[:mid], spec_b[mid:]
            spec = jnp.concatenate([ar * br - ai * bi, ar * bi + ai * br], axis=0)
            polar = dot(back_tab[...], spec)
            for s in range(2):
                in_buf[slot, q, :, :, i + s] = polar[:, s * LANES:(s + 1) * LANES].reshape(2, keep, LANES)

    def chain_stage(up, q):
        far = 0 if up else last
        slot = polar_slot(q)

        def hop(j):
            @pl.when(mine != far)
            def _():
                chain_copy(up, q, j).wait_recv()
                here = pl.ds(j * block, block)
                in_buf[slot, q, :, here] = in_buf[slot, q, :, here] + chain_buf[q, j + up]

            @pl.when(mine != j)
            def _():
                chain_copy(up, q, j).start()

        if up:
            each(0, last - mine + 1, lambda t: hop(last - t))
        else:
            each(0, mine + 1, hop)

    def final_stage(q):
        final_buf[q, :, :, share] = in_buf[polar_slot(q), q, :, pl.ds(me * kept, kept)]
        for side in range(sides):
            near_if(side, False, lambda: each(0, cores, lambda c: close_copy(side, q, c).start()))

    def out_stage(q):
        each(1, group, lambda d: out_copy(q, d).start())

    def halfway(side, q, value):
        half, tile = q // tiles, lax.rem(q, tiles)
        term = product(spread(value.reshape(count * group * ROWS, LANES)), right_tab[side, half])
        half_buf[side, :, tile] = half_buf[side, :, tile] + term.reshape(count, group, ROWS, width)

    def near_stage(q):
        each(1, group, lambda d: out_copy(q, d).wait_recv())
        for side in range(sides):
            near_if(side, False, lambda: each(1, chips, lambda d: near_copy(side, q, d).start()))
        halfway(0, q, final_buf[q])

    def screen_part(part):
        def one(item):
            terms = [
                stacked(half_buf[side, item, pl.ds(part * per_part, per_part)].reshape(PART, width))
                for side in range(1 + sides)
            ]
            total_buf[item] = total_buf[item] + product(left_tab[part], jnp.concatenate(terms, axis=0))

            @pl.when(part == parts - 1)
            def _():
                result_copy(item).start()

        each(0, count, one)

    def screen_stage(q):
        for side in range(sides):
            def arrived():
                each(0, cores, lambda c: close_wait(side, q, c))
                each(1, chips, lambda d: near_copy(side, q, d).wait_recv())
                halfway(1 + side, q, near_buf[side, q])
            near_if(side, True, arrived)
        done = q + 1 - (stages - tiles)

        @pl.when(jnp.logical_and(done > 0, lax.rem(done, per_part) == 0))
        def _():
            screen_part(done // per_part - 1)

    def by_kind(v, begin, body):
        for k in range(2):
            @pl.when(jnp.logical_and(lax.rem(v, 2) == k, jnp.logical_and(v >= begin, v < 2 * stages)))
            def _():
                body(k, v // 2)

    def clear():
        half_buf[...] = jnp.zeros(half_buf.shape, jnp.float32)
        total_buf[...] = jnp.zeros(total_buf.shape, jnp.float32)

    first, early = min(FIRST, 2 * tiles), min(EARLY, 2 * tiles)
    send_kind(0, 0)
    each(0, early // 2, lambda q: mate_kind(0, q))
    edge_copy().start()
    flip_half(0)
    each(1, first, lambda v: by_kind(v, 1, send_kind))
    each(0, early // 2, lambda q: mate_kind(1, q))
    clear()
    below = last - mine
    hops = jnp.maximum(mine, below)
    turn, quick = max(2 * stages - TURN, 0), max(stages - QUICK, 0)

    def ready(v):
        v = jnp.maximum(v, 0)
        count = jnp.where(v // 2 > quick, v // 2, jnp.minimum((v + 1) // 2 - 1, quick))
        return jnp.clip(count, 0, stages)

    def crossing(v):
        return jnp.minimum(ready(v - HOP * hops), jnp.maximum(v - turn + 1, 0) * BURST)

    def newly(counter, v, body):
        each(counter(v - 1), counter(v), body)

    def step(u):
        by_kind(u + AHEAD, first, send_kind)
        by_kind(u + early, early, mate_kind)
        by_kind(u, 0, forward_kind)
        for half in range(1, width // LANES):
            pl.when(u == 0)(lambda: flip_half(half))
        pl.when(u == 1)(prepare)
        newly(ready, u, compute_stage)
        newly(ready, u - HOP * mine, lambda q: chain_stage(1, q))
        newly(ready, u - HOP * below, lambda q: chain_stage(0, q))
        newly(ready, u - HOP * hops, final_stage)
        newly(crossing, u, out_stage)
        newly(crossing, u - NEAR, near_stage)
        newly(crossing, u - NEAR - SCREEN, screen_stage)

    length = max(2 * stages + HOP * last, turn + stages // BURST) + 2
    each(0, length + NEAR + SCREEN, step)

    def finish(q):
        for side in range(sides):
            near_if(side, False, lambda: each(0, cores, lambda c: close_copy(side, q, c).wait_send()))
            near_if(side, False, lambda: each(1, chips, lambda d: near_copy(side, q, d).wait_send()))
        for k in range(2):
            each(1, group, lambda d: in_copy(k, q, d).wait_send())

            @pl.when(jnp.logical_and(halo_sends(k, q), jnp.logical_not(slot_sent(q))) if k == 0 else halo_sends(k, q))
            def _():
                each(1, chips, lambda d: halo_copy(k, q, d).wait_send())

            @pl.when(halo_sends(k, q))
            def _():
                each(0, cores, lambda c: mate_copy(k, q, c).wait_send())
        each(mine + 1, groups, lambda j: chain_copy(1, q, j).wait_send())
        each(0, mine, lambda j: chain_copy(0, q, j).wait_send())
        each(1, group, lambda d: out_copy(q, d).wait_send())

    each(0, stages, finish)
    each(0, count, lambda item: result_copy(item).wait())


def local(g_lesser, g_greater, v_diag, v_upper):
    n, rows = lax.axis_size("energy"), lax.axis_size("space")
    sides = 1 if rows == 2 else 2
    _, held, _, size, width = g_lesser.shape
    keep = NW
    group = keep // held
    groups = n // group
    tiles = size // group // ROWS
    halves = width // LANES
    stages = tiles * halves
    kept = keep // n
    parts = size // PART
    cores = CORES if group % CORES == 0 else 1
    less = g_lesser.reshape(2, held, tiles, group, ROWS, width)
    great = g_greater.reshape(2, held, size, width)
    tabs = tables(keep)
    vmem_spec = pl.BlockSpec(memory_space=pltpu.VMEM)
    any_spec = pl.BlockSpec(memory_space=pl.ANY)
    dma = pltpu.SemaphoreType.DMA

    def vmem(*dims, dtype=jnp.float32):
        return pltpu.VMEM(dims, dtype)

    def tiled(*dims):
        return vmem(*dims, ROWS, LANES)

    out = pl.pallas_call(
        functools.partial(screening_kernel, n, group, rows),
        out_shape=jax.ShapeDtypeStruct((2 * kept, size, width), jnp.float32),
        in_specs=[vmem_spec] * (len(tabs) + 2) + [any_spec] * 2,
        out_specs=any_spec,
        scratch_shapes=[
            vmem(SLOTS, LANES, width),
            tiled(halves, 2, held, tiles, group),
            tiled(2, stages, 2, keep),
            tiled(stages, 2, keep),
            tiled(stages, groups + 1, 2, group * kept),
            tiled(stages, 2, kept, group),
            tiled(sides, stages, 2, kept, group),
            vmem(1 + sides, 2 * kept, tiles, group, ROWS, width),
            vmem(2 * kept, size, width),
            vmem(size, width),
            vmem(1 + sides, halves, 3 * LANES, width, dtype=jnp.bfloat16),
            vmem(parts, size, 3 * PART * (1 + sides), dtype=jnp.bfloat16),
            dma((SLOTS,)),
            dma((2, stages, group)), dma((2, stages, group)), dma((2, stages)),
            dma((2, stages, cores)), dma((stages, cores)),
            dma((2, stages, group // cores)), dma((stages, group // cores)),
            dma((2, stages, groups)), dma((2, stages, groups)),
            dma((stages, group)), dma((stages, group)),
            dma((sides, stages, cores)), dma((sides, stages, cores)),
            dma((sides, stages, group // cores)), dma((sides, stages, group // cores)),
            dma((2,)), dma((2 * kept,)),
        ],
        compiler_params=pltpu.CompilerParams(
            collective_id=0, has_side_effects=True, vmem_limit_bytes=2**26 - 2**16),
    )(*tabs, v_diag[0], v_upper[0], less, great)
    return out.reshape(2, kept, 1, size, width)


def solution(mesh):
    in_specs = (
        P(None, "energy", "space", None, None),
        P(None, "energy", "space", None, None),
        P("space", None, None),
        P("space", None, None),
    )
    out_specs = P(None, "energy", "space", None, None)
    return jax.shard_map(local, mesh=mesh, in_specs=in_specs, out_specs=out_specs, check_vma=False)
```
